16 devices in a mesh: dp: 2 (over y, z), sp: 8 (over x, core).
Axes of the slice: x: 4, y: 2, z: 1, core: 2. Of those that a mesh axis runs over, the one named last changes fastest.
The devices are a block of a 4x4x4 slice.
Arguments:
- q: bfloat16 [64, 32, 160], P('dp'), parts along dimension 0
- k: bfloat16 [64, 8192, 8, 160], P('dp', 'sp'), parts along dimension 0
- v: bfloat16 [64, 8192, 8, 160], P('dp', 'sp'), parts along dimension 0
Outputs:
- q: bfloat16 [64, 32, 160], P('dp'), parts along dimension 0
There are 2 independent parts. The reference program is written for one: setup_inputs(seed, part) draws one part's arguments, and reference() takes and returns one part's arrays. A program takes and returns all parts, laid end to end along the dimension named above; each array names one.
All inputs are finite; a program needn't handle non-finite values.
Results may differ from the reference program's by a relative error of at most 0.012.
Values are sent between devices in bfloat16 or wider.
A program may use at most 1.5 GiB of HBM per device.

```python
import jax
import jax.numpy as jnp

BATCH = 32
CACHE = 8192
HEADS = 32
KV_HEADS = 8
HEAD = 160


def setup_inputs(seed: int = 0, part: int = 0) -> dict:
    kq, kk, kv = (jax.random.fold_in(k, part) for k in jax.random.split(jax.random.key(seed), 3))
    return {
        "q": (3 * jax.random.normal(kq, (BATCH, HEADS, HEAD), jnp.float32)).astype(jnp.bfloat16),
        "k": jax.random.normal(kk, (BATCH, CACHE, KV_HEADS, HEAD), jnp.float32).astype(jnp.bfloat16),
        "v": jax.random.normal(kv, (BATCH, CACHE, KV_HEADS, HEAD), jnp.float32).astype(jnp.bfloat16),
    }


def einsum(form, a, b):
    return jnp.einsum(form, a.astype(jnp.float32), b.astype(jnp.float32))


def reference(q, k, v):
    grouped = q.reshape(BATCH, KV_HEADS, -1, HEAD)
    scores = einsum("bgsd,bugd->bgsu", grouped, k) * HEAD**-0.5
    weights = jax.nn.softmax(scores, -1).astype(jnp.bfloat16)
    return einsum("bgsu,bugd->bgsd", weights, v).astype(jnp.bfloat16).reshape(BATCH, HEADS, HEAD)
```

```python
import functools

import jax
import jax.numpy as jnp
from jax import lax
from jax.experimental import pallas as pl
from jax.experimental.pallas import tpu as pltpu
from jax.sharding import PartitionSpec as P

LANES = 128
RING = 6
LEAD = 3
LAG = 4
DIRECT = 2
PIECES = 2
LOG2E = 1.4426950408889634


def kernel(n, groups, q_hbm, k_hbm, v_hbm, out, q_in, spread, mask, q_wide, keys, values, weights, parts, stats, round_parts, round_stats, last_parts, last_stats,
           q_sem, k_sems, v_sems, tail_sems, part_send, stat_send, out_send, part_recv, stat_recv, out_recv, last_send, last_recv):
    sequences, width, _ = k_hbm.shape
    rows, head = q_hbm.shape
    heads = rows // sequences
    share = heads // groups
    last = sequences - 1
    shared = sequences - DIRECT
    piece = width // PIECES
    me = lax.axis_index("sp")
    peers = [{"sp": lax.rem(me + step, n)} for step in range(1, n)]

    def k_copy(i):
        return pltpu.make_async_copy(k_hbm.at[i], keys.at[lax.rem(i, RING)], k_sems.at[lax.rem(i, RING)])

    def v_copy(i):
        return pltpu.make_async_copy(v_hbm.at[i], values.at[lax.rem(i, RING)], v_sems.at[lax.rem(i, RING)])

    def tail_copy(p):
        at = pl.ds(piece * p, piece)
        return pltpu.make_async_copy(v_hbm.at[last, at], values.at[last % RING, at], tail_sems.at[p])

    def start_k(i):
        if isinstance(i, int):
            k_copy(i).start()
        else:
            pl.when(i < sequences)(lambda: k_copy(i).start())

    def start_v(i):
        if isinstance(i, int):
            v_copy(i).start()
            return
        pl.when(i < last)(lambda: v_copy(i).start())

        @pl.when(i == last)
        def _():
            for p in range(PIECES):
                tail_copy(p).start()

    def push(src, dst, send_sem, recv_sem, peer):
        pltpu.make_async_remote_copy(
            src_ref=src, dst_ref=dst, send_sem=send_sem, recv_sem=recv_sem, device_id=peer, device_id_type=pl.DeviceIdType.MESH
        ).start()

    def wait_for(ref, sem):
        pltpu.make_async_copy(ref, ref, sem).wait()

    def slot_of(i):
        return lax.rem(me - lax.rem(i, n) + n, n)

    def to_owner(i, src, dst, send_sem, recv_sem):
        slot = slot_of(i)

        @pl.when(slot > 0)
        def _():
            push(src.at[i], dst.at[lax.div(i, n), slot - 1], send_sem.at[i], recv_sem.at[lax.div(i, n)], {"sp": lax.rem(i, n)})

    def sent_to_owner(i, src, send_sem):
        pl.when(slot_of(i) > 0)(lambda: wait_for(src.at[i], send_sem.at[i]))

    def send_stats(i):
        to_owner(i, stats, round_stats, stat_send, stat_recv)

    def send_parts(i):
        to_owner(i, parts, round_parts, part_send, part_recv)

    def to_all(src, send_sem, recv_sem):
        for peer in peers:
            push(src, src, send_sem, recv_sem, peer)

    def tail_of(p):
        return pl.ds(heads // PIECES * p, heads // PIECES), last_send.at[DIRECT - 1 + p], last_recv.at[DIRECT - 1 + p]

    q_copy = pltpu.make_async_copy(q_hbm, q_in, q_sem)
    q_copy.start()
    for i in range(LEAD):
        k_copy(i).start()
    for i in range(LEAD, RING):
        k_copy(i).start()
        v_copy(i - LEAD).start()

    barrier = pltpu.get_barrier_semaphore()
    for peer in peers:
        pl.semaphore_signal(barrier, inc=1, device_id=peer, device_id_type=pl.DeviceIdType.MESH)

    column = lax.broadcasted_iota(jnp.int32, (8, width), 1)
    group = sum((column >= head * g).astype(jnp.int32) for g in range(1, groups))
    place = jnp.broadcast_to((column - head * group)[:1], (head, width))
    spread[...] = (lax.broadcasted_iota(jnp.int32, (head, width), 0) == place).astype(jnp.float32).astype(jnp.bfloat16)
    row = lax.broadcasted_iota(jnp.int32, (heads, width), 0) - share * jnp.broadcast_to(group[:1], (heads, width))
    mask[...] = jnp.logical_and(row >= 0, row < share).astype(jnp.float32).astype(jnp.bfloat16)

    q_copy.wait()
    few = 4 * heads

    def widen(i, _):
        at = pl.ds(pl.multiple_of(i * few, few), few)
        wide = jnp.dot(q_in[at, :], spread[...], preferred_element_type=jnp.float32).astype(jnp.bfloat16)
        q_wide[at, :] = wide * jnp.concatenate([mask[...]] * 4, 0)
        return 0

    lax.fori_loop(0, rows // few, widen, 0)

    lane = lax.broadcasted_iota(jnp.int32, (heads, LANES), 1)
    line = lax.broadcasted_iota(jnp.int32, (heads, LANES), 0)
    row8 = lax.broadcasted_iota(jnp.int32, (8, LANES), 0)
    factor = head**-0.5

    def weigh(i, direct=False):
        at = pl.ds(pl.multiple_of(i * heads, heads), heads)
        raw = jnp.dot(q_wide[at, :], keys[lax.rem(i, RING)], preferred_element_type=jnp.float32)
        high = jnp.max(raw, -1, keepdims=True)
        w = jnp.exp2((raw - high) * (factor * LOG2E))
        weights[lax.rem(i, LEAD + 1)] = w.astype(jnp.bfloat16)
        total = jnp.sum(w, -1, keepdims=True)
        both = jnp.where(lane == line, high * factor, 0.0) + jnp.where(lane == line + heads, total, 0.0)
        both = jnp.broadcast_to(jnp.sum(both, 0, keepdims=True), (8, LANES))
        if direct:
            last_stats[i - shared, me] = jnp.where(row8 == me, both, 0.0)
        else:
            stats[i] = jnp.where(row8 == slot_of(i), both, 0.0)

    def gather(i, w, first=0, count=None, direct=False):
        count = heads if count is None else count
        start = head * (first // share)
        size = head * (count // share)
        seen = lax.dot_general(
            w[first : first + count], values[lax.rem(i, RING), start : start + size], (((1,), (1,)), ((), ())), preferred_element_type=jnp.float32
        )
        upper = lax.broadcasted_iota(jnp.int32, (8, 2 * LANES), 0)
        blocks = []
        for top in range(0, count, 8):
            block = None
            for g in range(top // share, (top + 8) // share):
                begin = head * g
                base = min(begin // LANES * LANES, -(-size // LANES) * LANES - 2 * LANES)
                part = seen[top : top + 8, base : min(base + 2 * LANES, size)]
                if part.shape[1] < 2 * LANES:
                    part = jnp.concatenate([part, jnp.zeros((8, 2 * LANES - part.shape[1]), part.dtype)], 1)
                if begin > base:
                    part = pltpu.roll(part, 2 * LANES - (begin - base), 1)
                block = part if block is None else jnp.where(upper >= share * g - top, part, block)
            blocks.append(block)
        found = jnp.concatenate(blocks, 0).astype(jnp.bfloat16)
        if direct:
            last_parts[i - shared, me, first : first + count] = found
        else:
            parts[i] = found

    def scales(found):
        found = functools.reduce(lax.add, found)
        scale = jnp.exp(found - jnp.max(found, 0, keepdims=True))
        total = jnp.sum(pltpu.roll(found, LANES - heads, 1) * scale, 0, keepdims=True)
        scale = scale / total
        return [
            jnp.sum(jnp.where(lane == line, jnp.broadcast_to(scale[d : d + 1], (heads, LANES)), 0.0), -1, keepdims=True)
            for d in range(n)
        ]

    def join(i, factors, found):
        result = jnp.zeros((heads, 2 * LANES), jnp.float32)
        for d in range(n):
            result = result + found[d].astype(jnp.float32) * factors[d]
        out[i] = result[:, :head].astype(out.dtype)

    def join_own(r):
        i = n * r + me
        wait_for(round_stats.at[r], stat_recv.at[r])
        factors = scales([stats[i]] + [round_stats[r, d] for d in range(n - 1)])
        wait_for(round_parts.at[r], part_recv.at[r])
        join(i, factors, [parts[i]] + [round_parts[r, d] for d in range(n - 1)])
        to_all(out.at[i], out_send.at[r], out_recv.at[r])

    for i in range(LEAD):
        k_copy(i).wait()
        weigh(i)
        start_k(i + RING)
        start_v(i + RING - LEAD)
    pl.semaphore_wait(barrier, n - 1)
    for i in range(LEAD - 1):
        send_stats(i)

    def step(i, follows=True, direct=False, first=False):
        if follows:
            start_k(i + LEAD + RING - 1)
            start_v(i + RING - 1)

            @pl.when(jnp.logical_and(lax.rem(i, n) == LAG, i > n))
            def _():
                join_own(lax.div(i, n) - 1)

            send_parts(i - 1)
        k_copy(i + LEAD).wait()
        v_copy(i).wait()
        if not direct or first:
            send_stats(i + LEAD - 1)
        w = weights[lax.rem(i, LEAD + 1)]
        weigh(i + LEAD, direct)
        gather(i, w)

    def body(i, _):
        step(i)
        return 0

    step(0, follows=False)
    lax.fori_loop(1, shared - LEAD, body, 0)
    for i in range(shared - LEAD, sequences - LEAD):
        step(jnp.int32(i), direct=True, first=i == shared - LEAD)
        to_all(last_stats.at[i + LEAD - shared, me], stat_send.at[i + LEAD], last_recv.at[DIRECT + PIECES - 1 + i + LEAD - shared])

    send_parts(last - LEAD)
    for i in range(sequences - LEAD, last):
        v_copy(i).wait()
        gather(i, weights[i % (LEAD + 1)], direct=i >= shared)
        if i < shared:
            send_parts(i)
        else:
            to_all(last_parts.at[i - shared, me], last_send.at[i - shared], last_recv.at[i - shared])
    w = weights[last % (LEAD + 1)]
    for p in range(PIECES):
        tail_copy(p).wait()
        gather(last, w, heads // PIECES * p, heads // PIECES, direct=True)
        at, send_sem, recv_sem = tail_of(p)
        to_all(last_parts.at[DIRECT - 1, me, at], send_sem, recv_sem)

    rounds = -(-shared // n)
    owners = shared - n * (rounds - 1)
    pl.when(me < owners)(lambda: join_own(rounds - 1))

    for i in range(shared, last):
        d = i - shared
        wait_for(last_stats.at[d, pl.ds(0, n - 1)], last_recv.at[DIRECT + PIECES - 1 + d])
        factors = scales([last_stats[d, e] for e in range(n)])
        wait_for(last_parts.at[d, pl.ds(0, n - 1)], last_recv.at[d])
        join(i, factors, [last_parts[d, e] for e in range(n)])
    d = DIRECT - 1
    wait_for(last_stats.at[d, pl.ds(0, n - 1)], last_recv.at[DIRECT + PIECES - 1 + d])
    factors = scales([last_stats[d, e] for e in range(n)])
    for p in range(PIECES):
        at, send_sem, recv_sem = tail_of(p)
        wait_for(last_parts.at[d, pl.ds(0, n - 1), at], recv_sem)
    join(last, factors, [last_parts[d, e] for e in range(n)])

    def drain(i, _):
        sent_to_owner(i, stats, stat_send)
        sent_to_owner(i, parts, part_send)
        return 0

    lax.fori_loop(0, shared, drain, 0)
    for i in range(shared, sequences):
        wait_for(last_stats.at[i - shared, pl.ds(0, n - 1)], stat_send.at[i])
        if i < last:
            wait_for(last_parts.at[i - shared, pl.ds(0, n - 1)], last_send.at[i - shared])
    for p in range(PIECES):
        at, send_sem, recv_sem = tail_of(p)
        wait_for(last_parts.at[DIRECT - 1, pl.ds(0, n - 1), at], send_sem)
    for r in range(rounds):
        each = n if r < rounds - 1 else owners

        @pl.when(me < each)
        def _():
            wait_for(out.at[pl.ds(n * r, n - 1)], out_send.at[r])
            wait_for(out.at[pl.ds(n * r, each - 1)], out_recv.at[r])

        @pl.when(me >= each)
        def _():
            wait_for(out.at[pl.ds(n * r, each)], out_recv.at[r])


def attend(n, q, k, v):
    sequences, heads, head = q.shape
    tokens, groups = k.shape[1:3]
    width = groups * head
    rounds = -(-(sequences - DIRECT) // n)
    k, v = (jnp.transpose(x, (0, 2, 3, 1)).reshape(sequences, width, tokens) for x in (k, v))
    return pl.pallas_call(
        functools.partial(kernel, n, groups),
        out_shape=pltpu.VMEM(q.shape, q.dtype),
        in_specs=[pl.BlockSpec(memory_space=pl.ANY)] * 3,
        out_specs=pl.BlockSpec(memory_space=pltpu.VMEM),
        scratch_shapes=[
            pltpu.VMEM((sequences * heads, head), jnp.bfloat16),
            pltpu.VMEM((head, width), jnp.bfloat16),
            pltpu.VMEM((heads, width), jnp.bfloat16),
            pltpu.VMEM((sequences * heads, width), jnp.bfloat16),
            pltpu.VMEM((RING, width, tokens), jnp.bfloat16),
            pltpu.VMEM((RING, width, tokens), jnp.bfloat16),
            pltpu.VMEM((LEAD + 1, heads, tokens), jnp.bfloat16),
            pltpu.VMEM((sequences - DIRECT, heads, 2 * LANES), jnp.bfloat16),
            pltpu.VMEM((sequences - DIRECT, 8, LANES), jnp.float32),
            pltpu.VMEM((rounds, n - 1, heads, 2 * LANES), jnp.bfloat16),
            pltpu.VMEM((rounds, n - 1, 8, LANES), jnp.float32),
            pltpu.VMEM((DIRECT, n, heads, 2 * LANES), jnp.bfloat16),
            pltpu.VMEM((DIRECT, n, 8, LANES), jnp.float32),
            pltpu.SemaphoreType.DMA,
            pltpu.SemaphoreType.DMA((RING,)),
            pltpu.SemaphoreType.DMA((RING,)),
            pltpu.SemaphoreType.DMA((PIECES,)),
            pltpu.SemaphoreType.DMA((sequences,)),
            pltpu.SemaphoreType.DMA((sequences,)),
            pltpu.SemaphoreType.DMA((rounds,)),
            pltpu.SemaphoreType.DMA((rounds,)),
            pltpu.SemaphoreType.DMA((rounds,)),
            pltpu.SemaphoreType.DMA((rounds,)),
            pltpu.SemaphoreType.DMA((DIRECT + PIECES - 1,)),
            pltpu.SemaphoreType.DMA((2 * DIRECT + PIECES - 1,)),
        ],
        compiler_params=pltpu.CompilerParams(collective_id=0, has_side_effects=True, vmem_limit_bytes=56 * 2**20),
        name="attend",
    )(q.reshape(sequences * heads, head), k, v)


def solution(mesh):
    return jax.shard_map(
        functools.partial(attend, mesh.shape["sp"]),
        mesh=mesh,
        in_specs=(P("dp", None, None), P("dp", "sp", None, None), P("dp", "sp", None, None)),
        out_specs=P("dp", None, None),
        check_vma=False,
    )
```

```python
import functools

import jax
import jax.numpy as jnp
from jax import lax
from jax.experimental import pallas as pl
from jax.experimental.pallas import tpu as pltpu
from jax.sharding import PartitionSpec as P

LANES = 128
RING = 6
LEAD = 1
LAG = 3
DIRECT = 3
PIECES = 2
LOG2E = 1.4426950408889634


def kernel(n, groups, q_hbm, k_hbm, v_hbm, out, q_in, spread, mask, q_wide, keys, values, weights, parts, stats, round_parts, round_stats, last_parts, last_stats,
           q_sem, k_sems, v_sems, tail_sems, part_send, stat_send, out_send, part_recv, stat_recv, out_recv, last_send, last_recv, last_stat_send, last_stat_recv):
    sequences, width, _ = k_hbm.shape
    rows, head = q_hbm.shape
    heads = rows // sequences
    share = heads // groups
    last = sequences - 1
    shared = sequences - DIRECT
    piece = width // PIECES
    few = heads // PIECES
    rest = head - LANES
    me = lax.axis_index("sp")
    peers = [{"sp": lax.rem(me + step, n)} for step in range(1, n)]

    def k_copy(i):
        return pltpu.make_async_copy(k_hbm.at[i], keys.at[lax.rem(i, RING)], k_sems.at[lax.rem(i, RING)])

    def v_copy(i):
        return pltpu.make_async_copy(v_hbm.at[i], values.at[lax.rem(i, RING)], v_sems.at[lax.rem(i, RING)])

    def tail_copy(p):
        at = pl.ds(piece * p, piece)
        return pltpu.make_async_copy(v_hbm.at[last, at], values.at[last % RING, at], tail_sems.at[p])

    def start_k(i):
        if not isinstance(i, int):
            pl.when(i < sequences)(lambda: k_copy(i).start(priority=1))
        elif i < sequences:
            k_copy(i).start(priority=1)

    def start_v(i):
        def whole():
            v_copy(i).start(priority=1)

        def pieces():
            for p in range(PIECES):
                tail_copy(p).start(priority=1)

        if not isinstance(i, int):
            pl.when(i < last)(whole)
            pl.when(i == last)(pieces)
        elif i <= last:
            (whole if i < last else pieces)()

    def push(src, dst, send_sem, recv_sem, peer):
        pltpu.make_async_remote_copy(
            src_ref=src, dst_ref=dst, send_sem=send_sem, recv_sem=recv_sem, device_id=peer, device_id_type=pl.DeviceIdType.MESH
        ).start()

    def wait_for(ref, sem):
        pltpu.make_async_copy(ref, ref, sem).wait()

    def slot_of(i):
        return lax.rem(me - lax.rem(i, n) + n, n)

    def to_owner(i, src, dst, send_sem, recv_sem):
        slot = slot_of(i)
        r = lax.div(i, n)

        @pl.when(slot > 0)
        def _():
            push(src.at[i], dst.at[r, slot - 1], send_sem.at[r], recv_sem.at[r], {"sp": lax.rem(i, n)})

    def send_stats(i):
        if isinstance(i, int) and i >= shared:
            to_all(last_stats.at[i - shared, me], last_stat_send.at[i - shared], last_stat_recv.at[i - shared])
        else:
            to_owner(i, stats, round_stats, stat_send, stat_recv)

    def send_parts(i):
        if isinstance(i, int) and i >= shared:
            to_all(last_parts.at[i - shared, me], last_send.at[i - shared], last_recv.at[i - shared])
        else:
            to_owner(i, parts, round_parts, part_send, part_recv)

    def to_all(src, send_sem, recv_sem):
        for peer in peers:
            push(src, src, send_sem, recv_sem, peer)

    def tail_of(p):
        return last_send.at[DIRECT - 1 + p], last_recv.at[DIRECT - 1 + p]

    q_copy = pltpu.make_async_copy(q_hbm, q_in, q_sem)
    q_copy.start()
    for i in range(LEAD):
        k_copy(i).start(priority=1)
    for i in range(LEAD, RING):
        k_copy(i).start(priority=1)
        v_copy(i - LEAD).start(priority=1)

    barrier = pltpu.get_barrier_semaphore()
    for peer in peers:
        pl.semaphore_signal(barrier, inc=1, device_id=peer, device_id_type=pl.DeviceIdType.MESH)

    column = lax.broadcasted_iota(jnp.int32, (8, width), 1)
    group = sum((column >= head * g).astype(jnp.int32) for g in range(1, groups))
    place = jnp.broadcast_to((column - head * group)[:1], (head, width))
    spread[...] = (lax.broadcasted_iota(jnp.int32, (head, width), 0) == place).astype(jnp.float32).astype(jnp.bfloat16)
    row = lax.broadcasted_iota(jnp.int32, (heads, width), 0) - share * jnp.broadcast_to(group[:1], (heads, width))
    mask[...] = jnp.logical_and(row >= 0, row < share).astype(jnp.float32).astype(jnp.bfloat16)

    q_copy.wait()
    many = 4 * heads

    def widen(i, _):
        at = pl.ds(pl.multiple_of(i * many, many), many)
        wide = jnp.dot(q_in[at, :], spread[...], preferred_element_type=jnp.float32).astype(jnp.bfloat16)
        q_wide[at, :] = wide * jnp.concatenate([mask[...]] * 4, 0)
        return 0

    lax.fori_loop(0, rows // many, widen, 0)

    lane = lax.broadcasted_iota(jnp.int32, (heads, LANES), 1)
    line = lax.broadcasted_iota(jnp.int32, (heads, LANES), 0)
    row8 = lax.broadcasted_iota(jnp.int32, (8, LANES), 0)
    lane8 = lax.broadcasted_iota(jnp.int32, (8, LANES), 1)
    factor = head**-0.5

    def weigh(i):
        direct = isinstance(i, int) and i >= shared
        at = pl.ds(pl.multiple_of(i * heads, heads), heads)
        raw = jnp.dot(q_wide[at, :], keys[lax.rem(i, RING)], preferred_element_type=jnp.float32)
        high = jnp.max(raw, -1, keepdims=True)
        w = jnp.exp2((raw - high) * (factor * LOG2E))
        weights[lax.rem(i, LEAD + 1)] = w.astype(jnp.bfloat16)
        total = jnp.sum(w, -1, keepdims=True)
        both = jnp.where(lane == line, high * factor, 0.0) + jnp.where(lane == line + heads, total, 0.0)
        both = jnp.sum(both, 0, keepdims=True)
        if direct:
            last_stats[i - shared, me] = both
        else:
            stats[i] = jnp.where(row8 == slot_of(i), jnp.broadcast_to(both, (8, LANES)), 0.0)

    def gather(i, w, first=0, count=None):
        count = heads if count is None else count
        start = head * (first // share)
        size = head * (count // share)
        seen = lax.dot_general(
            w[first : first + count], values[lax.rem(i, RING), start : start + size], (((1,), (1,)), ((), ())), preferred_element_type=jnp.float32
        )
        upper = lax.broadcasted_iota(jnp.int32, (8, 2 * LANES), 0)
        blocks = []
        for top in range(0, count, 8):
            block = None
            for g in range(top // share, (top + 8) // share):
                begin = head * g
                base = min(begin // LANES * LANES, -(-size // LANES) * LANES - 2 * LANES)
                part = seen[top : top + 8, base : min(base + 2 * LANES, size)]
                if part.shape[1] < 2 * LANES:
                    part = jnp.concatenate([part, jnp.zeros((8, 2 * LANES - part.shape[1]), part.dtype)], 1)
                if begin > base:
                    part = pltpu.roll(part, 2 * LANES - (begin - base), 1)
                block = part if block is None else jnp.where(upper >= share * g - top, part, block)
            blocks.append(block)
        if isinstance(i, int) and i >= shared:
            for p in range(count // few):
                pack = pack_rows(blocks[few // 8 * p : few // 8 * (p + 1)])
                last_parts[i - shared, me, first // few + p] = pack.astype(jnp.bfloat16)
        else:
            parts[i] = jnp.concatenate(blocks, 0).astype(jnp.bfloat16)

    def pack_rows(blocks):
        over = blocks[0][:, LANES:]
        for j, block in enumerate(blocks[1:], 1):
            over = jnp.where(lane8 >= rest * j, pltpu.roll(block[:, LANES:], rest * j, 1), over)
        return jnp.concatenate([block[:, :LANES] for block in blocks] + [over], 0)

    def join_packed(i, factors):
        for p in range(PIECES):
            result = jnp.zeros((few + 8, LANES), jnp.float32)
            for e in range(n):
                weight = jnp.broadcast_to(factors[e][few * p : few * (p + 1)], (few, LANES))
                blocks = [weight[8 * j : 8 * j + 8] for j in range(few // 8)]
                over = blocks[0]
                for j, block in enumerate(blocks[1:], 1):
                    over = jnp.where(lane8 >= rest * j, block, over)
                result = result + last_parts[i - shared, e, p].astype(jnp.float32) * jnp.concatenate(blocks + [over], 0)
            out[i, few * p : few * (p + 1), :LANES] = result[:few].astype(out.dtype)
            over = [result[few:]] + [pltpu.roll(result[few:], LANES - rest * j, 1) for j in range(1, few // 8)]
            out[i, few * p : few * (p + 1), LANES:] = jnp.concatenate(over, 0)[:, :rest].astype(out.dtype)

    def last_scales(d):
        return scales([jnp.where(row8 == e, jnp.broadcast_to(last_stats[d, e], (8, LANES)), 0.0) for e in range(n)])

    def scales(found):
        found = functools.reduce(lax.add, found)
        scale = jnp.exp(found - jnp.max(found, 0, keepdims=True))
        total = jnp.sum(pltpu.roll(found, LANES - heads, 1) * scale, 0, keepdims=True)
        scale = scale / total
        return [
            jnp.sum(jnp.where(lane == line, jnp.broadcast_to(scale[d : d + 1], (heads, LANES)), 0.0), -1, keepdims=True)
            for d in range(n)
        ]

    def join(i, factors, found):
        result = jnp.zeros((heads, 2 * LANES), jnp.float32)
        for d in range(n):
            result = result + found[d].astype(jnp.float32) * factors[d]
        out[i] = result[:, :head].astype(out.dtype)

    def join_own(r):
        i = n * r + me
        wait_for(round_stats.at[r], stat_recv.at[r])
        factors = scales([stats[i]] + [round_stats[r, d] for d in range(n - 1)])
        wait_for(round_parts.at[r], part_recv.at[r])
        join(i, factors, [parts[i]] + [round_parts[r, d] for d in range(n - 1)])
        to_all(out.at[i], out_send.at[r], out_recv.at[r])

    for i in range(LEAD):
        k_copy(i).wait()
        weigh(i)
        start_k(i + RING)
        start_v(i + RING - LEAD)
    pl.semaphore_wait(barrier, n - 1)
    for i in range(LEAD - 1):
        send_stats(i)

    def step(i, first=False):
        if not first:
            start_k(i + LEAD + RING - 1)
            start_v(i + RING - 1)
            if not isinstance(i, int):
                pl.when(jnp.logical_and(lax.rem(i, n) == LAG, i > n))(lambda: join_own(lax.div(i, n) - 1))
            elif i % n == LAG and i > n:
                join_own(i // n - 1)
            send_parts(i - 1)
        send_stats(i + LEAD - 1)
        k_copy(i + LEAD).wait()
        v_copy(i).wait()
        w = weights[lax.rem(i, LEAD + 1)]
        weigh(i + LEAD)
        gather(i, w)

    def body(i, _):
        step(i)
        return 0

    step(0, first=True)
    lax.fori_loop(1, shared - LEAD, body, 0)
    for i in range(shared - LEAD, sequences - LEAD):
        step(i)

    send_stats(last)
    send_parts(last - LEAD)
    for i in range(sequences - LEAD, last):
        v_copy(i).wait()
        gather(i, weights[i % (LEAD + 1)])
        send_parts(i)
    w = weights[last % (LEAD + 1)]
    for p in range(PIECES):
        tail_copy(p).wait()
        gather(last, w, few * p, few)
        to_all(last_parts.at[DIRECT - 1, me, p], *tail_of(p))

    rounds = -(-shared // n)
    owners = shared - n * (rounds - 1)
    pl.when(me < owners)(lambda: join_own(rounds - 1))

    def each_round(r, own, other):
        if n * (r + 1) <= shared:
            own(n)
        else:
            pl.when(me < owners)(lambda: own(owners))
            pl.when(me >= owners)(lambda: other(owners))

    for r in range(rounds):

        def sent(count):
            if count:
                wait_for(stats.at[pl.ds(n * r, count)], stat_send.at[r])
                wait_for(parts.at[pl.ds(n * r, count)], part_send.at[r])

        each_round(r, lambda count: sent(count - 1), sent)
    for d in range(DIRECT):
        wait_for(last_stats.at[d, pl.ds(0, n - 1)], last_stat_send.at[d])

    for d in range(DIRECT - 1):
        wait_for(last_stats.at[d, pl.ds(0, n - 1)], last_stat_recv.at[d])
        factors = last_scales(d)
        wait_for(last_parts.at[d, pl.ds(0, n - 1)], last_send.at[d])
        wait_for(last_parts.at[d, pl.ds(0, n - 1)], last_recv.at[d])
        join_packed(shared + d, factors)
    d = DIRECT - 1
    wait_for(last_stats.at[d, pl.ds(0, n - 1)], last_stat_recv.at[d])
    factors = last_scales(d)
    for p in range(PIECES):
        for sem in tail_of(p):
            wait_for(last_parts.at[d, pl.ds(0, n - 1), p], sem)
    join_packed(last, factors)

    for r in range(rounds):

        def sent(count):
            wait_for(out.at[pl.ds(0, n - 1)], out_send.at[r])
            wait_for(out.at[pl.ds(0, count - 1)], out_recv.at[r])

        each_round(r, sent, lambda count: wait_for(out.at[pl.ds(0, count)], out_recv.at[r]))


def attend(n, q, k, v):
    sequences, heads, head = q.shape
    tokens, groups = k.shape[1:3]
    width = groups * head
    rounds = -(-(sequences - DIRECT) // n)
    k, v = (jnp.transpose(x, (0, 2, 3, 1)).reshape(sequences, width, tokens) for x in (k, v))
    return pl.pallas_call(
        functools.partial(kernel, n, groups),
        out_shape=pltpu.VMEM(q.shape, q.dtype),
        in_specs=[pl.BlockSpec(memory_space=pl.ANY)] * 3,
        out_specs=pl.BlockSpec(memory_space=pltpu.VMEM),
        scratch_shapes=[
            pltpu.VMEM((sequences * heads, head), jnp.bfloat16),
            pltpu.VMEM((head, width), jnp.bfloat16),
            pltpu.VMEM((heads, width), jnp.bfloat16),
            pltpu.VMEM((sequences * heads, width), jnp.bfloat16),
            pltpu.VMEM((RING, width, tokens), jnp.bfloat16),
            pltpu.VMEM((RING, width, tokens), jnp.bfloat16),
            pltpu.VMEM((LEAD + 1, heads, tokens), jnp.bfloat16),
            pltpu.VMEM((sequences - DIRECT, heads, 2 * LANES), jnp.bfloat16),
            pltpu.VMEM((sequences - DIRECT, 8, LANES), jnp.float32),
            pltpu.VMEM((rounds, n - 1, heads, 2 * LANES), jnp.bfloat16),
            pltpu.VMEM((rounds, n - 1, 8, LANES), jnp.float32),
            pltpu.VMEM((DIRECT, n, PIECES, heads // PIECES + 8, LANES), jnp.bfloat16),
            pltpu.VMEM((DIRECT, n, 1, LANES), jnp.float32),
            pltpu.SemaphoreType.DMA,
            pltpu.SemaphoreType.DMA((RING,)),
            pltpu.SemaphoreType.DMA((RING,)),
            pltpu.SemaphoreType.DMA((PIECES,)),
            *[pltpu.SemaphoreType.DMA((rounds,))] * 6,
            *[pltpu.SemaphoreType.DMA((DIRECT + PIECES - 1,))] * 2,
            *[pltpu.SemaphoreType.DMA((DIRECT,))] * 2,
        ],
        compiler_params=pltpu.CompilerParams(collective_id=0, has_side_effects=True, vmem_limit_bytes=56 * 2**20),
        name="attend",
    )(q.reshape(sequences * heads, head), k, v)


def solution(mesh):
    return jax.shard_map(
        functools.partial(attend, mesh.shape["sp"]),
        mesh=mesh,
        in_specs=(P("dp", None, None), P("dp", "sp", None, None), P("dp", "sp", None, None)),
        out_specs=P("dp", None, None),
        check_vma=False,
    )
```

```python
import functools

import jax
import jax.numpy as jnp
from jax import lax
from jax.experimental import pallas as pl
from jax.experimental.pallas import tpu as pltpu
from jax.sharding import PartitionSpec as P

LANES = 128
RING = 6
LEAD = 1
LAG = 3
DIRECT = 4
PIECES = 1
LOG2E = 1.4426950408889634


def kernel(n, groups, q_hbm, k_hbm, v_hbm, out, q_in, spread, mask, q_wide, keys, values, weights, parts, stats, round_parts, round_stats, last_parts, last_stats,
           q_sem, k_sems, v_sems, tail_sems, part_send, stat_send, out_send, part_recv, stat_recv, out_recv, last_send, last_recv, last_stat_send, last_stat_recv):
    sequences, width, _ = k_hbm.shape
    rows, head = q_hbm.shape
    heads = rows // sequences
    share = heads // groups
    last = sequences - 1
    shared = sequences - DIRECT
    rounds = -(-shared // n)
    owners = shared - n * (rounds - 1)
    piece = width // PIECES
    few = heads // PIECES
    rest = head - LANES
    me = lax.axis_index("sp")
    peers = [{"sp": lax.rem(me + step, n)} for step in sorted(range(1, n), key=lambda step: -min(step, n - step))]

    def k_copy(i):
        return pltpu.make_async_copy(k_hbm.at[i], keys.at[lax.rem(i, RING)], k_sems.at[lax.rem(i, RING)])

    def v_copy(i):
        return pltpu.make_async_copy(v_hbm.at[i], values.at[lax.rem(i, RING)], v_sems.at[lax.rem(i, RING)])

    def tail_copy(p):
        at = pl.ds(piece * p, piece)
        return pltpu.make_async_copy(v_hbm.at[last, at], values.at[last % RING, at], tail_sems.at[p])

    def start_k(i):
        if not isinstance(i, int):
            pl.when(i < sequences)(lambda: k_copy(i).start(priority=1))
        elif i < sequences:
            k_copy(i).start(priority=1)

    def start_v(i):
        def whole():
            v_copy(i).start(priority=1)

        def pieces():
            for p in range(PIECES):
                tail_copy(p).start(priority=1)

        if not isinstance(i, int):
            pl.when(i < last)(whole)
            pl.when(i == last)(pieces)
        elif i <= last:
            (whole if i < last else pieces)()

    def push(src, dst, send_sem, recv_sem, peer):
        pltpu.make_async_remote_copy(
            src_ref=src, dst_ref=dst, send_sem=send_sem, recv_sem=recv_sem, device_id=peer, device_id_type=pl.DeviceIdType.MESH
        ).start()

    def wait_for(ref, sem):
        pltpu.make_async_copy(ref, ref, sem).wait()

    def slot_of(i):
        return lax.rem(me - lax.rem(i, n) + n, n)

    def to_owner(i, src, dst, send_sem, recv_sem):
        slot = slot_of(i)
        r = lax.div(i, n)

        @pl.when(slot > 0)
        def _():
            push(src.at[i], dst.at[r, slot - 1], send_sem.at[r], recv_sem.at[r], {"sp": lax.rem(i, n)})

    def send_stats(i):
        if isinstance(i, int) and i == last:
            to_all(last_stats.at[me], last_stat_send, last_stat_recv)
        elif not isinstance(i, int) or i < shared:
            to_owner(i, stats, round_stats, stat_send, stat_recv)

    def send_parts(i):
        if isinstance(i, int) and i >= shared:
            to_all(last_parts.at[i - shared, me], last_send.at[i - shared], last_recv.at[i - shared])
        else:
            to_owner(i, parts, round_parts, part_send, part_recv)

    def to_all(src, send_sem, recv_sem):
        for peer in peers:
            push(src, src, send_sem, recv_sem, peer)

    def tail_of(p):
        return last_send.at[DIRECT - 1 + p], last_recv.at[DIRECT - 1 + p]

    q_copy = pltpu.make_async_copy(q_hbm, q_in, q_sem)
    q_copy.start()
    for i in range(LEAD):
        k_copy(i).start(priority=1)
    for i in range(LEAD, RING):
        k_copy(i).start(priority=1)
        v_copy(i - LEAD).start(priority=1)

    barrier = pltpu.get_barrier_semaphore()
    for peer in peers:
        pl.semaphore_signal(barrier, inc=1, device_id=peer, device_id_type=pl.DeviceIdType.MESH)

    column = lax.broadcasted_iota(jnp.int32, (8, width), 1)
    group = sum((column >= head * g).astype(jnp.int32) for g in range(1, groups))
    place = jnp.broadcast_to((column - head * group)[:1], (head, width))
    spread[...] = (lax.broadcasted_iota(jnp.int32, (head, width), 0) == place).astype(jnp.float32).astype(jnp.bfloat16)
    row = lax.broadcasted_iota(jnp.int32, (heads, width), 0) - share * jnp.broadcast_to(group[:1], (heads, width))
    mask[...] = jnp.logical_and(row >= 0, row < share).astype(jnp.float32).astype(jnp.bfloat16)

    q_copy.wait()
    many = 4 * heads

    def widen(i, _):
        at = pl.ds(pl.multiple_of(i * many, many), many)
        wide = jnp.dot(q_in[at, :], spread[...], preferred_element_type=jnp.float32).astype(jnp.bfloat16)
        q_wide[at, :] = wide * jnp.concatenate([mask[...]] * 4, 0)
        return 0

    lax.fori_loop(0, rows // many, widen, 0)

    lane = lax.broadcasted_iota(jnp.int32, (heads, LANES), 1)
    line = lax.broadcasted_iota(jnp.int32, (heads, LANES), 0)
    row8 = lax.broadcasted_iota(jnp.int32, (8, LANES), 0)
    lane8 = lax.broadcasted_iota(jnp.int32, (8, LANES), 1)
    factor = head**-0.5

    def weigh(i):
        direct = isinstance(i, int) and i >= shared
        at = pl.ds(pl.multiple_of(i * heads, heads), heads)
        raw = jnp.dot(q_wide[at, :], keys[lax.rem(i, RING)], preferred_element_type=jnp.float32)
        high = jnp.max(raw, -1, keepdims=True)
        w = jnp.exp2((raw - high) * (factor * LOG2E))
        weights[lax.rem(i, LEAD + 1)] = w.astype(jnp.bfloat16)
        total = jnp.sum(w, -1, keepdims=True)
        both = jnp.where(lane == line, high * factor, 0.0) + jnp.where(lane == line + heads, total, 0.0)
        both = jnp.sum(both, 0, keepdims=True)
        if direct:
            last_stats[me, i - shared] = both
        else:
            stats[i] = jnp.where(row8 == slot_of(i), jnp.broadcast_to(both, (8, LANES)), 0.0)

    def gather(i, w, first=0, count=heads):
        start = head * (first // share)
        size = head * (count // share)
        tokens = w.shape[1]
        w = w[first : first + count]

        def dot(begin, end, cut=slice(0, tokens)):
            block = values[lax.rem(i, RING), start + begin : start + end, cut]
            return lax.dot_general(w[:, cut], block, (((1,), (1,)), ((), ())), preferred_element_type=jnp.float32)

        even = size // (4 * LANES) * (4 * LANES) if isinstance(i, int) and i == last else size
        seen, more = dot(0, even), None
        if even < size:
            seen = jnp.concatenate([seen, dot(even, size, slice(0, tokens // 2))], 1)
            more = dot(even, size, slice(tokens // 2, tokens))

        def taken(top, shift_of):
            block = None
            for g in range(top // share, (top + 8) // share):
                begin = head * g
                base = min(begin // LANES * LANES, size - 2 * LANES)
                shift = shift_of(begin - base) % (2 * LANES)
                part = seen[top : top + 8, base : base + 2 * LANES]
                part = pltpu.roll(part, shift, 1) if shift else part
                if base + 2 * LANES > even:
                    extra = more[top : top + 8, max(base - even, 0) : base + 2 * LANES - even]
                    if base < even:
                        extra = jnp.concatenate([jnp.zeros((8, even - base), extra.dtype), extra], 1)
                    part = part + (pltpu.roll(extra, shift, 1) if shift else extra)
                block = part if block is None else jnp.where(upper >= share * g - top, part, block)
            return block

        upper = lax.broadcasted_iota(jnp.int32, (8, 2 * LANES), 0)
        tops = range(0, count, 8)
        if isinstance(i, int) and i >= shared:
            for p in range(count // few):
                blocks, over = [], None
                for j, top in enumerate(tops[few // 8 * p : few // 8 * (p + 1)]):
                    blocks.append(taken(top, lambda column: -column)[:, :LANES])
                    beside = taken(top, lambda column: rest * j - column - LANES)[:, :LANES]
                    over = beside if over is None else jnp.where(lane8 >= rest * j, beside, over)
                last_parts[i - shared, me, first // few + p] = jnp.concatenate(blocks + [over], 0).astype(jnp.bfloat16)
        else:
            parts[i] = jnp.concatenate([taken(top, lambda column: -column) for top in tops], 0).astype(jnp.bfloat16)

    def join_packed(i, factors):
        for p in range(PIECES):
            result = jnp.zeros((few + 8, LANES), jnp.float32)
            for e in range(n):
                weight = jnp.broadcast_to(factors[e][few * p : few * (p + 1)], (few, LANES))
                blocks = [weight[8 * j : 8 * j + 8] for j in range(few // 8)]
                over = blocks[0]
                for j, block in enumerate(blocks[1:], 1):
                    over = jnp.where(lane8 >= rest * j, block, over)
                result = result + last_parts[i - shared, e, p].astype(jnp.float32) * jnp.concatenate(blocks + [over], 0)
            out[i, few * p : few * (p + 1), :LANES] = result[:few].astype(out.dtype)
            over = [result[few:]] + [pltpu.roll(result[few:], LANES - rest * j, 1) for j in range(1, few // 8)]
            out[i, few * p : few * (p + 1), LANES:] = jnp.concatenate(over, 0)[:, :rest].astype(out.dtype)

    def last_scales(d):
        return scales([jnp.where(row8 == e, jnp.broadcast_to(last_stats[e, d], (8, LANES)), 0.0) for e in range(n)])

    def scales(found):
        found = functools.reduce(lax.add, found)
        scale = jnp.exp(found - jnp.max(found, 0, keepdims=True))
        total = jnp.sum(pltpu.roll(found, LANES - heads, 1) * scale, 0, keepdims=True)
        scale = scale / total
        return [
            jnp.sum(jnp.where(lane == line, jnp.broadcast_to(scale[d : d + 1], (heads, LANES)), 0.0), -1, keepdims=True)
            for d in range(n)
        ]

    def join(i, factors, found):
        result = jnp.zeros((heads, 2 * LANES), jnp.float32)
        for d in range(n):
            result = result + found[d].astype(jnp.float32) * factors[d]
        out[i] = result[:, :head].astype(out.dtype)

    def join_own(r):
        i = n * r + me
        wait_for(round_stats.at[r], stat_recv.at[r])
        factors = scales([stats[i]] + [round_stats[r, d] for d in range(n - 1)])
        wait_for(round_parts.at[r], part_recv.at[r])
        join(i, factors, [parts[i]] + [round_parts[r, d] for d in range(n - 1)])
        to_all(out.at[i], out_send.at[r], out_recv.at[r])

    for i in range(LEAD):
        k_copy(i).wait()
        weigh(i)
        start_k(i + RING)
        start_v(i + RING - LEAD)
    pl.semaphore_wait(barrier, n - 1)
    for i in range(LEAD - 1):
        send_stats(i)

    def step(i, first=False):
        if not first:
            start_k(i + LEAD + RING - 1)
            start_v(i + RING - 1)
            if not isinstance(i, int):
                pl.when(jnp.logical_and(lax.rem(i, n) == LAG, i > n))(lambda: join_own(lax.div(i, n) - 1))
            elif i % n == LAG and i > n:
                join_own(i // n - 1)
            send_parts(i - 1)
        send_stats(i + LEAD - 1)
        k_copy(i + LEAD).wait()
        v_copy(i).wait()
        w = weights[lax.rem(i, LEAD + 1)]
        weigh(i + LEAD)
        gather(i, w)

    def body(i, _):
        step(i)
        return 0

    step(0, first=True)
    lax.fori_loop(1, shared - LEAD, body, 0)
    for i in range(shared - LEAD, sequences - LEAD):
        step(i)

    send_stats(last)
    send_parts(last - LEAD)
    for i in range(sequences - LEAD, last):
        v_copy(i).wait()
        gather(i, weights[i % (LEAD + 1)])
        send_parts(i)
    w = weights[last % (LEAD + 1)]
    for p in range(PIECES):
        tail_copy(p).wait()
        gather(last, w, few * p, few)
        to_all(last_parts.at[DIRECT - 1, me, p], *tail_of(p))

    pl.when(me < owners)(lambda: join_own(rounds - 1))

    def each_round(r, own, other):
        if n * (r + 1) <= shared:
            own(n)
        else:
            pl.when(me < owners)(lambda: own(owners))
            pl.when(me >= owners)(lambda: other(owners))

    for r in range(rounds):

        def sent(count):
            if count:
                wait_for(stats.at[pl.ds(n * r, count)], stat_send.at[r])
                wait_for(parts.at[pl.ds(n * r, count)], part_send.at[r])

        each_round(r, lambda count: sent(count - 1), sent)
    for sem in (last_stat_send, last_stat_recv):
        wait_for(last_stats.at[pl.ds(0, n - 1)], sem)

    for d in range(DIRECT - 1):
        factors = last_scales(d)
        wait_for(last_parts.at[d, pl.ds(0, n - 1)], last_send.at[d])
        wait_for(last_parts.at[d, pl.ds(0, n - 1)], last_recv.at[d])
        join_packed(shared + d, factors)
    d = DIRECT - 1
    factors = last_scales(d)
    for p in range(PIECES):
        for sem in tail_of(p):
            wait_for(last_parts.at[d, pl.ds(0, n - 1), p], sem)
    join_packed(last, factors)

    for r in range(rounds):

        def sent(count):
            wait_for(out.at[pl.ds(0, n - 1)], out_send.at[r])
            wait_for(out.at[pl.ds(0, count - 1)], out_recv.at[r])

        each_round(r, sent, lambda count: wait_for(out.at[pl.ds(0, count)], out_recv.at[r]))


def attend(n, q, k, v):
    sequences, heads, head = q.shape
    tokens, groups = k.shape[1:3]
    width = groups * head
    rounds = -(-(sequences - DIRECT) // n)
    k, v = (jnp.transpose(x, (0, 2, 3, 1)).reshape(sequences, width, tokens) for x in (k, v))
    return pl.pallas_call(
        functools.partial(kernel, n, groups),
        out_shape=pltpu.VMEM(q.shape, q.dtype),
        in_specs=[pl.BlockSpec(memory_space=pl.ANY)] * 3,
        out_specs=pl.BlockSpec(memory_space=pltpu.VMEM),
        scratch_shapes=[
            pltpu.VMEM((sequences * heads, head), jnp.bfloat16),
            pltpu.VMEM((head, width), jnp.bfloat16),
            pltpu.VMEM((heads, width), jnp.bfloat16),
            pltpu.VMEM((sequences * heads, width), jnp.bfloat16),
            pltpu.VMEM((RING, width, tokens), jnp.bfloat16),
            pltpu.VMEM((RING, width, tokens), jnp.bfloat16),
            pltpu.VMEM((LEAD + 1, heads, tokens), jnp.bfloat16),
            pltpu.VMEM((sequences - DIRECT, heads, 2 * LANES), jnp.bfloat16),
            pltpu.VMEM((sequences - DIRECT, 8, LANES), jnp.float32),
            pltpu.VMEM((rounds, n - 1, heads, 2 * LANES), jnp.bfloat16),
            pltpu.VMEM((rounds, n - 1, 8, LANES), jnp.float32),
            pltpu.VMEM((DIRECT, n, PIECES, heads // PIECES + 8, LANES), jnp.bfloat16),
            pltpu.VMEM((n, DIRECT, 1, LANES), jnp.float32),
            pltpu.SemaphoreType.DMA,
            pltpu.SemaphoreType.DMA((RING,)),
            pltpu.SemaphoreType.DMA((RING,)),
            pltpu.SemaphoreType.DMA((PIECES,)),
            *[pltpu.SemaphoreType.DMA((rounds,))] * 6,
            *[pltpu.SemaphoreType.DMA((DIRECT + PIECES - 1,))] * 2,
            *[pltpu.SemaphoreType.DMA] * 2,
        ],
        compiler_params=pltpu.CompilerParams(collective_id=0, has_side_effects=True, vmem_limit_bytes=56 * 2**20),
        name="attend",
    )(q.reshape(sequences * heads, head), k, v)


def solution(mesh):
    return jax.shard_map(
        functools.partial(attend, mesh.shape["sp"]),
        mesh=mesh,
        in_specs=(P("dp", None, None), P("dp", "sp", None, None), P("dp", "sp", None, None)),
        out_specs=P("dp", None, None),
        check_vma=False,
    )
```

```python
import functools

import jax
import jax.numpy as jnp
from jax import lax
from jax.experimental import pallas as pl
from jax.experimental.pallas import tpu as pltpu
from jax.sharding import PartitionSpec as P

LANES = 128
RING = 6
LEAD = 1
LAG = 2
DIRECT = 4
PIECES = 1
LOG2E = 1.4426950408889634


def kernel(n, groups, q_hbm, k_hbm, v_hbm, out, q_in, spread, mask, q_wide, keys, values, weights, parts, stats, round_parts, round_stats, last_parts, last_stats,
           q_sem, k_sems, v_sems, tail_sems, part_send, stat_send, out_send, part_recv, stat_recv, out_recv, last_send, last_recv, last_stat_send, last_stat_recv):
    sequences, width, _ = k_hbm.shape
    rows, head = q_hbm.shape
    heads = rows // sequences
    share = heads // groups
    last = sequences - 1
    shared = sequences - DIRECT
    rounds = -(-shared // n)
    owners = shared - n * (rounds - 1)
    piece = width // PIECES
    few = heads // PIECES
    rest = head - LANES
    me = lax.axis_index("sp")
    peers = [{"sp": lax.rem(me + step, n)} for step in sorted(range(1, n), key=lambda step: -min(step, n - step))]

    def k_copy(i):
        return pltpu.make_async_copy(k_hbm.at[i], keys.at[lax.rem(i, RING)], k_sems.at[lax.rem(i, RING)])

    def v_copy(i):
        return pltpu.make_async_copy(v_hbm.at[i], values.at[lax.rem(i, RING)], v_sems.at[lax.rem(i, RING)])

    def tail_copy(p):
        at = pl.ds(piece * p, piece)
        return pltpu.make_async_copy(v_hbm.at[last, at], values.at[last % RING, at], tail_sems.at[p])

    def start_k(i):
        if not isinstance(i, int):
            pl.when(i < sequences)(lambda: k_copy(i).start(priority=1))
        elif i < sequences:
            k_copy(i).start(priority=1)

    def start_v(i):
        def whole():
            v_copy(i).start(priority=1)

        def pieces():
            for p in range(PIECES):
                tail_copy(p).start(priority=1)

        if not isinstance(i, int):
            pl.when(i < last)(whole)
            pl.when(i == last)(pieces)
        elif i <= last:
            (whole if i < last else pieces)()

    def push(src, dst, send_sem, recv_sem, peer):
        pltpu.make_async_remote_copy(
            src_ref=src, dst_ref=dst, send_sem=send_sem, recv_sem=recv_sem, device_id=peer, device_id_type=pl.DeviceIdType.MESH
        ).start()

    def wait_for(ref, sem):
        pltpu.make_async_copy(ref, ref, sem).wait()

    def slot_of(i):
        return lax.rem(me - lax.rem(i, n) + n, n)

    def to_owner(i, src, dst, send_sem, recv_sem):
        slot = slot_of(i)
        r = lax.div(i, n)

        @pl.when(slot > 0)
        def _():
            push(src.at[i], dst.at[r, slot - 1], send_sem.at[r], recv_sem.at[r], {"sp": lax.rem(i, n)})

    def send_stats(i):
        if isinstance(i, int) and i == last:
            to_all(last_stats.at[me], last_stat_send, last_stat_recv)
        elif not isinstance(i, int) or i < shared:
            to_owner(i, stats, round_stats, stat_send, stat_recv)

    def send_parts(i):
        if isinstance(i, int) and i >= shared:
            to_all(last_parts.at[i - shared, me], last_send.at[i - shared], last_recv.at[i - shared])
        else:
            to_owner(i, parts, round_parts, part_send, part_recv)

    def to_all(src, send_sem, recv_sem):
        for peer in peers:
            push(src, src, send_sem, recv_sem, peer)

    def tail_of(p):
        return last_send.at[DIRECT - 1 + p], last_recv.at[DIRECT - 1 + p]

    q_copy = pltpu.make_async_copy(q_hbm, q_in, q_sem)
    q_copy.start()
    for i in range(LEAD):
        k_copy(i).start(priority=1)
    for i in range(LEAD, RING):
        k_copy(i).start(priority=1)
        v_copy(i - LEAD).start(priority=1)

    barrier = pltpu.get_barrier_semaphore()
    for peer in peers:
        pl.semaphore_signal(barrier, inc=1, device_id=peer, device_id_type=pl.DeviceIdType.MESH)

    column = lax.broadcasted_iota(jnp.int32, (8, width), 1)
    group = sum((column >= head * g).astype(jnp.int32) for g in range(1, groups))
    place = jnp.broadcast_to((column - head * group)[:1], (head, width))
    spread[...] = (lax.broadcasted_iota(jnp.int32, (head, width), 0) == place).astype(jnp.float32).astype(jnp.bfloat16)
    row = lax.broadcasted_iota(jnp.int32, (heads, width), 0) - share * jnp.broadcast_to(group[:1], (heads, width))
    mask[...] = jnp.logical_and(row >= 0, row < share).astype(jnp.float32).astype(jnp.bfloat16)

    q_copy.wait()
    many = 4 * heads

    def widen(i, _):
        at = pl.ds(pl.multiple_of(i * many, many), many)
        wide = jnp.dot(q_in[at, :], spread[...], preferred_element_type=jnp.float32).astype(jnp.bfloat16)
        q_wide[at, :] = wide * jnp.concatenate([mask[...]] * 4, 0)
        return 0

    lax.fori_loop(0, rows // many, widen, 0)

    lane = lax.broadcasted_iota(jnp.int32, (heads, LANES), 1)
    line = lax.broadcasted_iota(jnp.int32, (heads, LANES), 0)
    row8 = lax.broadcasted_iota(jnp.int32, (8, LANES), 0)
    lane8 = lax.broadcasted_iota(jnp.int32, (8, LANES), 1)
    factor = head**-0.5

    def weigh(i):
        direct = isinstance(i, int) and i >= shared
        at = pl.ds(pl.multiple_of(i * heads, heads), heads)
        raw = jnp.dot(q_wide[at, :], keys[lax.rem(i, RING)], preferred_element_type=jnp.float32)
        high = jnp.max(raw, -1, keepdims=True)
        w = jnp.exp2((raw - high) * (factor * LOG2E))
        weights[lax.rem(i, LEAD + 1)] = w.astype(jnp.bfloat16)
        total = jnp.sum(w, -1, keepdims=True)
        both = jnp.where(lane == line, high * factor, 0.0) + jnp.where(lane == line + heads, total, 0.0)
        both = jnp.sum(both, 0, keepdims=True)
        if direct:
            last_stats[me, i - shared] = both
        else:
            stats[i] = jnp.where(row8 == slot_of(i), jnp.broadcast_to(both, (8, LANES)), 0.0)

    def gather(i, w, first=0, count=heads):
        start = head * (first // share)
        size = head * (count // share)
        tokens = w.shape[1]
        w = w[first : first + count]

        def dot(begin, end, cut=slice(0, tokens)):
            block = values[lax.rem(i, RING), start + begin : start + end, cut]
            return lax.dot_general(w[:, cut], block, (((1,), (1,)), ((), ())), preferred_element_type=jnp.float32)

        even = size // (4 * LANES) * (4 * LANES)
        seen, more = dot(0, even), None
        if even < size:
            seen = jnp.concatenate([seen, dot(even, size, slice(0, tokens // 2))], 1)
            more = dot(even, size, slice(tokens // 2, tokens))

        def taken(top, shift_of):
            block = None
            for g in range(top // share, (top + 8) // share):
                begin = head * g
                base = min(begin // LANES * LANES, size - 2 * LANES)
                shift = shift_of(begin - base) % (2 * LANES)
                part = seen[top : top + 8, base : base + 2 * LANES]
                part = pltpu.roll(part, shift, 1) if shift else part
                if base + 2 * LANES > even:
                    extra = more[top : top + 8, max(base - even, 0) : base + 2 * LANES - even]
                    if base < even:
                        extra = jnp.concatenate([jnp.zeros((8, even - base), extra.dtype), extra], 1)
                    part = part + (pltpu.roll(extra, shift, 1) if shift else extra)
                block = part if block is None else jnp.where(upper >= share * g - top, part, block)
            return block

        upper = lax.broadcasted_iota(jnp.int32, (8, 2 * LANES), 0)
        tops = range(0, count, 8)
        if isinstance(i, int) and i >= shared:
            for p in range(count // few):
                blocks, over = [], None
                for j, top in enumerate(tops[few // 8 * p : few // 8 * (p + 1)]):
                    blocks.append(taken(top, lambda column: -column)[:, :LANES])
                    beside = taken(top, lambda column: rest * j - column - LANES)[:, :LANES]
                    over = beside if over is None else jnp.where(lane8 >= rest * j, beside, over)
                last_parts[i - shared, me, first // few + p] = jnp.concatenate(blocks + [over], 0).astype(jnp.bfloat16)
        else:
            parts[i] = jnp.concatenate([taken(top, lambda column: -column) for top in tops], 0).astype(jnp.bfloat16)

    def join_packed(i, factors):
        for p in range(PIECES):
            result = jnp.zeros((few + 8, LANES), jnp.float32)
            for e in range(n):
                weight = jnp.broadcast_to(factors[e][few * p : few * (p + 1)], (few, LANES))
                blocks = [weight[8 * j : 8 * j + 8] for j in range(few // 8)]
                over = blocks[0]
                for j, block in enumerate(blocks[1:], 1):
                    over = jnp.where(lane8 >= rest * j, block, over)
                result = result + last_parts[i - shared, e, p].astype(jnp.float32) * jnp.concatenate(blocks + [over], 0)
            out[i, few * p : few * (p + 1), :LANES] = result[:few].astype(out.dtype)
            over = [result[few:]] + [pltpu.roll(result[few:], LANES - rest * j, 1) for j in range(1, few // 8)]
            out[i, few * p : few * (p + 1), LANES:] = jnp.concatenate(over, 0)[:, :rest].astype(out.dtype)

    def last_scales(d):
        return scales([jnp.where(row8 == e, jnp.broadcast_to(last_stats[e, d], (8, LANES)), 0.0) for e in range(n)])

    def scales(found):
        found = functools.reduce(lax.add, found)
        scale = jnp.exp(found - jnp.max(found, 0, keepdims=True))
        total = jnp.sum(pltpu.roll(found, LANES - heads, 1) * scale, 0, keepdims=True)
        scale = scale / total
        return [
            jnp.sum(jnp.where(lane == line, jnp.broadcast_to(scale[d : d + 1], (heads, LANES)), 0.0), -1, keepdims=True)
            for d in range(n)
        ]

    def join(i, factors, found):
        result = jnp.zeros((heads, 2 * LANES), jnp.float32)
        for d in range(n):
            result = result + found[d].astype(jnp.float32) * factors[d]
        out[i] = result[:, :head].astype(out.dtype)

    def join_own(r):
        i = n * r + me
        wait_for(round_stats.at[r], stat_recv.at[r])
        factors = scales([stats[i]] + [round_stats[r, d] for d in range(n - 1)])
        wait_for(round_parts.at[r], part_recv.at[r])
        join(i, factors, [parts[i]] + [round_parts[r, d] for d in range(n - 1)])
        to_all(out.at[i], out_send.at[r], out_recv.at[r])

    for i in range(LEAD):
        k_copy(i).wait()
        weigh(i)
        start_k(i + RING)
        start_v(i + RING - LEAD)
    pl.semaphore_wait(barrier, n - 1)
    for i in range(LEAD - 1):
        send_stats(i)

    def step(i, first=False):
        if not first:
            start_k(i + LEAD + RING - 1)
            start_v(i + RING - 1)
            if not isinstance(i, int):
                pl.when(jnp.logical_and(lax.rem(i, n) == LAG, i > n))(lambda: join_own(lax.div(i, n) - 1))
            elif i % n == LAG and i > n:
                join_own(i // n - 1)
            send_parts(i - 1)
        send_stats(i + LEAD - 1)
        k_copy(i + LEAD).wait()
        v_copy(i).wait()
        w = weights[lax.rem(i, LEAD + 1)]
        weigh(i + LEAD)
        gather(i, w)

    def body(i, _):
        step(i)
        return 0

    step(0, first=True)
    lax.fori_loop(1, shared - LEAD, body, 0)
    for i in range(shared - LEAD, sequences - LEAD):
        step(i)

    send_stats(last)
    send_parts(last - LEAD)
    for i in range(sequences - LEAD, last):
        v_copy(i).wait()
        gather(i, weights[i % (LEAD + 1)])
        send_parts(i)
    w = weights[last % (LEAD + 1)]
    for p in range(PIECES):
        tail_copy(p).wait()
        gather(last, w, few * p, few)
        to_all(last_parts.at[DIRECT - 1, me, p], *tail_of(p))

    pl.when(me < owners)(lambda: join_own(rounds - 1))

    def each_round(r, own, other):
        if n * (r + 1) <= shared:
            own(n)
        else:
            pl.when(me < owners)(lambda: own(owners))
            pl.when(me >= owners)(lambda: other(owners))

    for r in range(rounds):

        def sent(count):
            if count:
                wait_for(stats.at[pl.ds(n * r, count)], stat_send.at[r])
                wait_for(parts.at[pl.ds(n * r, count)], part_send.at[r])

        each_round(r, lambda count: sent(count - 1), sent)
    for sem in (last_stat_send, last_stat_recv):
        wait_for(last_stats.at[pl.ds(0, n - 1)], sem)

    for d in range(DIRECT - 1):
        factors = last_scales(d)
        wait_for(last_parts.at[d, pl.ds(0, n - 1)], last_send.at[d])
        wait_for(last_parts.at[d, pl.ds(0, n - 1)], last_recv.at[d])
        join_packed(shared + d, factors)
    d = DIRECT - 1
    factors = last_scales(d)
    for p in range(PIECES):
        for sem in tail_of(p):
            wait_for(last_parts.at[d, pl.ds(0, n - 1), p], sem)
    join_packed(last, factors)

    for r in range(rounds):

        def sent(count):
            wait_for(out.at[pl.ds(0, n - 1)], out_send.at[r])
            wait_for(out.at[pl.ds(0, count - 1)], out_recv.at[r])

        each_round(r, sent, lambda count: wait_for(out.at[pl.ds(0, count)], out_recv.at[r]))


def attend(n, q, k, v):
    sequences, heads, head = q.shape
    tokens, groups = k.shape[1:3]
    width = groups * head
    rounds = -(-(sequences - DIRECT) // n)
    k, v = (jnp.transpose(x, (0, 2, 3, 1)).reshape(sequences, width, tokens) for x in (k, v))
    return pl.pallas_call(
        functools.partial(kernel, n, groups),
        out_shape=pltpu.VMEM(q.shape, q.dtype),
        in_specs=[pl.BlockSpec(memory_space=pl.ANY)] * 3,
        out_specs=pl.BlockSpec(memory_space=pltpu.VMEM),
        scratch_shapes=[
            pltpu.VMEM((sequences * heads, head), jnp.bfloat16),
            pltpu.VMEM((head, width), jnp.bfloat16),
            pltpu.VMEM((heads, width), jnp.bfloat16),
            pltpu.VMEM((sequences * heads, width), jnp.bfloat16),
            pltpu.VMEM((RING, width, tokens), jnp.bfloat16),
            pltpu.VMEM((RING, width, tokens), jnp.bfloat16),
            pltpu.VMEM((LEAD + 1, heads, tokens), jnp.bfloat16),
            pltpu.VMEM((sequences - DIRECT, heads, 2 * LANES), jnp.bfloat16),
            pltpu.VMEM((sequences - DIRECT, 8, LANES), jnp.float32),
            pltpu.VMEM((rounds, n - 1, heads, 2 * LANES), jnp.bfloat16),
            pltpu.VMEM((rounds, n - 1, 8, LANES), jnp.float32),
            pltpu.VMEM((DIRECT, n, PIECES, heads // PIECES + 8, LANES), jnp.bfloat16),
            pltpu.VMEM((n, DIRECT, 1, LANES), jnp.float32),
            pltpu.SemaphoreType.DMA,
            pltpu.SemaphoreType.DMA((RING,)),
            pltpu.SemaphoreType.DMA((RING,)),
            pltpu.SemaphoreType.DMA((PIECES,)),
            *[pltpu.SemaphoreType.DMA((rounds,))] * 6,
            *[pltpu.SemaphoreType.DMA((DIRECT + PIECES - 1,))] * 2,
            *[pltpu.SemaphoreType.DMA] * 2,
        ],
        compiler_params=pltpu.CompilerParams(collective_id=0, has_side_effects=True, vmem_limit_bytes=56 * 2**20),
        name="attend",
    )(q.reshape(sequences * heads, head), k, v)


def solution(mesh):
    return jax.shard_map(
        functools.partial(attend, mesh.shape["sp"]),
        mesh=mesh,
        in_specs=(P("dp", None, None), P("dp", "sp", None, None), P("dp", "sp", None, None)),
        out_specs=P("dp", None, None),
        check_vma=False,
    )
```

```python
import functools

import jax
import jax.numpy as jnp
from jax import lax
from jax.experimental import pallas as pl
from jax.experimental.pallas import tpu as pltpu
from jax.sharding import PartitionSpec as P

LANES = 128
RING = 6
LEAD = 1
LAG = 2
DIRECT = 4
PIECES = 1
LOG2E = 1.4426950408889634


def kernel(n, groups, q_hbm, k_hbm, v_hbm, out, q_in, spread, mask, q_wide, keys, values, weights, parts, stats, round_parts, round_stats, last_parts, last_stats,
           q_sem, k_sems, v_sems, tail_sems, part_send, stat_send, out_send, part_recv, stat_recv, out_recv, last_send, last_recv, last_stat_send, last_stat_recv):
    sequences, width, _ = k_hbm.shape
    rows, head = q_hbm.shape
    heads = rows // sequences
    share = heads // groups
    last = sequences - 1
    shared = sequences - DIRECT
    rounds = -(-shared // n)
    owners = shared - n * (rounds - 1)
    piece = width // PIECES
    few = heads // PIECES
    rest = head - LANES
    me = lax.axis_index("sp")
    peers = [{"sp": lax.rem(me + step, n)} for step in sorted(range(1, n), key=lambda step: -min(step, n - step))]

    def k_copy(i):
        return pltpu.make_async_copy(k_hbm.at[i], keys.at[lax.rem(i, RING)], k_sems.at[lax.rem(i, RING)])

    def v_copy(i):
        return pltpu.make_async_copy(v_hbm.at[i], values.at[lax.rem(i, RING)], v_sems.at[lax.rem(i, RING)])

    def tail_copy(p):
        at = pl.ds(piece * p, piece)
        return pltpu.make_async_copy(v_hbm.at[last, at], values.at[last % RING, at], tail_sems.at[p])

    def start_k(i):
        if not isinstance(i, int):
            pl.when(i < sequences)(lambda: k_copy(i).start(priority=1))
        elif i < sequences:
            k_copy(i).start(priority=1)

    def start_v(i):
        def whole():
            v_copy(i).start(priority=1)

        def pieces():
            for p in range(PIECES):
                tail_copy(p).start(priority=1)

        if not isinstance(i, int):
            pl.when(i < last)(whole)
            pl.when(i == last)(pieces)
        elif i <= last:
            (whole if i < last else pieces)()

    def push(src, dst, send_sem, recv_sem, peer):
        pltpu.make_async_remote_copy(
            src_ref=src, dst_ref=dst, send_sem=send_sem, recv_sem=recv_sem, device_id=peer, device_id_type=pl.DeviceIdType.MESH
        ).start()

    def wait_for(ref, sem):
        pltpu.make_async_copy(ref, ref, sem).wait()

    def slot_of(i):
        return lax.rem(me - lax.rem(i, n) + n, n)

    def to_owner(i, src, dst, send_sem, recv_sem):
        slot = slot_of(i)
        r = lax.div(i, n)

        @pl.when(slot > 0)
        def _():
            push(src.at[i], dst.at[r, slot - 1], send_sem.at[r], recv_sem.at[r], {"sp": lax.rem(i, n)})

    def send_stats(i):
        if isinstance(i, int) and i == last:
            to_all(last_stats.at[me], last_stat_send, last_stat_recv)
        elif not isinstance(i, int) or i < shared:
            to_owner(i, stats, round_stats, stat_send, stat_recv)

    def send_parts(i):
        if isinstance(i, int) and i >= shared:
            to_all(last_parts.at[i - shared, me], last_send.at[i - shared], last_recv.at[i - shared])
        else:
            to_owner(i, parts, round_parts, part_send, part_recv)

    def to_all(src, send_sem, recv_sem):
        for peer in peers:
            push(src, src, send_sem, recv_sem, peer)

    def tail_of(p):
        return last_send.at[DIRECT - 1 + p], last_recv.at[DIRECT - 1 + p]

    q_copy = pltpu.make_async_copy(q_hbm, q_in, q_sem)
    q_copy.start()
    for i in range(LEAD):
        k_copy(i).start(priority=1)
    for i in range(LEAD, RING):
        k_copy(i).start(priority=1)
        v_copy(i - LEAD).start(priority=1)

    barrier = pltpu.get_barrier_semaphore()
    for peer in peers:
        pl.semaphore_signal(barrier, inc=1, device_id=peer, device_id_type=pl.DeviceIdType.MESH)

    column = lax.broadcasted_iota(jnp.int32, (8, width), 1)
    group = sum((column >= head * g).astype(jnp.int32) for g in range(1, groups))
    place = jnp.broadcast_to((column - head * group)[:1], (head, width))
    spread[...] = (lax.broadcasted_iota(jnp.int32, (head, width), 0) == place).astype(jnp.float32).astype(jnp.bfloat16)
    row = lax.broadcasted_iota(jnp.int32, (heads, width), 0) - share * jnp.broadcast_to(group[:1], (heads, width))
    mask[...] = jnp.logical_and(row >= 0, row < share).astype(jnp.float32).astype(jnp.bfloat16)

    q_copy.wait()
    many = 4 * heads

    def widen(i, _):
        at = pl.ds(pl.multiple_of(i * many, many), many)
        wide = jnp.dot(q_in[at, :], spread[...], preferred_element_type=jnp.float32).astype(jnp.bfloat16)
        q_wide[at, :] = wide * jnp.concatenate([mask[...]] * 4, 0)
        return 0

    lax.fori_loop(0, rows // many, widen, 0)

    lane = lax.broadcasted_iota(jnp.int32, (heads, LANES), 1)
    line = lax.broadcasted_iota(jnp.int32, (heads, LANES), 0)
    row8 = lax.broadcasted_iota(jnp.int32, (8, LANES), 0)
    lane8 = lax.broadcasted_iota(jnp.int32, (8, LANES), 1)
    factor = head**-0.5

    def weigh(i):
        direct = isinstance(i, int) and i >= shared
        at = pl.ds(pl.multiple_of(i * heads, heads), heads)
        raw = jnp.dot(q_wide[at, :], keys[lax.rem(i, RING)], preferred_element_type=jnp.float32)
        high = jnp.max(raw, -1, keepdims=True)
        w = jnp.exp2((raw - high) * (factor * LOG2E))
        weights[lax.rem(i, LEAD + 1)] = w.astype(jnp.bfloat16)
        total = jnp.sum(w, -1, keepdims=True)
        both = jnp.where(lane == line, high * factor, 0.0) + jnp.where(lane == line + heads, total, 0.0)
        both = jnp.sum(both, 0, keepdims=True)
        if direct:
            last_stats[me, i - shared] = both
        else:
            stats[i] = jnp.where(row8 == slot_of(i), jnp.broadcast_to(both, (8, LANES)), 0.0)

    def gather(i, w, first=0, count=heads):
        start = head * (first // share)
        size = head * (count // share)
        tokens = w.shape[1]
        w = w[first : first + count]

        def dot(begin, end, cut=slice(0, tokens)):
            block = values[lax.rem(i, RING), start + begin : start + end, cut]
            return lax.dot_general(w[:, cut], block, (((1,), (1,)), ((), ())), preferred_element_type=jnp.float32)

        even = size // (4 * LANES) * (4 * LANES)
        seen, more = dot(0, even), None
        if even < size:
            seen = jnp.concatenate([seen, dot(even, size, slice(0, tokens // 2))], 1)
            more = dot(even, size, slice(tokens // 2, tokens))

        def taken(top, shift_of):
            block = None
            for g in range(top // share, (top + 8) // share):
                begin = head * g
                base = min(begin // LANES * LANES, size - 2 * LANES)
                shift = shift_of(begin - base) % (2 * LANES)
                part = seen[top : top + 8, base : base + 2 * LANES]
                part = pltpu.roll(part, shift, 1) if shift else part
                if base + 2 * LANES > even:
                    extra = more[top : top + 8, max(base - even, 0) : base + 2 * LANES - even]
                    if base < even:
                        extra = jnp.concatenate([jnp.zeros((8, even - base), extra.dtype), extra], 1)
                    part = part + (pltpu.roll(extra, shift, 1) if shift else extra)
                block = part if block is None else jnp.where(upper >= share * g - top, part, block)
            return block

        upper = lax.broadcasted_iota(jnp.int32, (8, 2 * LANES), 0)
        tops = range(0, count, 8)
        if isinstance(i, int) and i >= shared:
            for p in range(count // few):
                blocks, over = [], None
                for j, top in enumerate(tops[few // 8 * p : few // 8 * (p + 1)]):
                    blocks.append(taken(top, lambda column: -column)[:, :LANES])
                    beside = taken(top, lambda column: rest * j - column - LANES)[:, :LANES]
                    over = beside if over is None else jnp.where(lane8 >= rest * j, beside, over)
                last_parts[i - shared, me, first // few + p] = jnp.concatenate(blocks + [over], 0).astype(jnp.bfloat16)
        else:
            parts[i] = jnp.concatenate([taken(top, lambda column: -column) for top in tops], 0).astype(jnp.bfloat16)

    def join_packed(i, factors):
        for p in range(PIECES):
            result = jnp.zeros((few + 8, LANES), jnp.float32)
            for e in range(n):
                weight = jnp.broadcast_to(factors[e][few * p : few * (p + 1)], (few, LANES))
                blocks = [weight[8 * j : 8 * j + 8] for j in range(few // 8)]
                over = blocks[0]
                for j, block in enumerate(blocks[1:], 1):
                    over = jnp.where(lane8 >= rest * j, block, over)
                result = result + last_parts[i - shared, e, p].astype(jnp.float32) * jnp.concatenate(blocks + [over], 0)
            out[i, few * p : few * (p + 1), :LANES] = result[:few].astype(out.dtype)
            over = [result[few:]] + [pltpu.roll(result[few:], LANES - rest * j, 1) for j in range(1, few // 8)]
            out[i, few * p : few * (p + 1), LANES:] = jnp.concatenate(over, 0)[:, :rest].astype(out.dtype)

    def last_scales(d):
        return scales([jnp.where(row8 == e, jnp.broadcast_to(last_stats[e, d], (8, LANES)), 0.0) for e in range(n)])

    def scales(found):
        found = functools.reduce(lax.add, found)
        scale = jnp.exp(found - jnp.max(found, 0, keepdims=True))
        total = jnp.sum(pltpu.roll(found, LANES - heads, 1) * scale, 0, keepdims=True)
        scale = scale / total
        return [
            jnp.sum(jnp.where(lane == line, jnp.broadcast_to(scale[d : d + 1], (heads, LANES)), 0.0), -1, keepdims=True)
            for d in range(n)
        ]

    def join(i, factors, found):
        result = jnp.zeros((heads, 2 * LANES), jnp.float32)
        for d in range(n):
            result = result + found[d].astype(jnp.float32) * factors[d]
        out[i] = result[:, :head].astype(out.dtype)

    def join_own(r):
        i = n * r + me
        wait_for(round_stats.at[r], stat_recv.at[r])
        factors = scales([stats[i]] + [round_stats[r, d] for d in range(n - 1)])
        wait_for(round_parts.at[r], part_recv.at[r])
        join(i, factors, [parts[i]] + [round_parts[r, d] for d in range(n - 1)])
        to_all(out.at[i], out_send.at[r], out_recv.at[r])

    for i in range(LEAD):
        k_copy(i).wait()
        weigh(i)
        start_k(i + RING)
        start_v(i + RING - LEAD)
    pl.semaphore_wait(barrier, n - 1)
    for i in range(LEAD - 1):
        send_stats(i)

    def step(i, first=False):
        if not first:
            start_k(i + LEAD + RING - 1)
            start_v(i + RING - 1)
            if not isinstance(i, int):
                pl.when(jnp.logical_and(lax.rem(i, n) == LAG, i > n))(lambda: join_own(lax.div(i, n) - 1))
            elif i % n == LAG and i > n:
                join_own(i // n - 1)
            elif i == last - LEAD:
                pl.when(me < owners)(lambda: join_own(rounds - 1))
            send_parts(i - 1)
        send_stats(i + LEAD - 1)
        k_copy(i + LEAD).wait()
        v_copy(i).wait()
        w = weights[lax.rem(i, LEAD + 1)]
        weigh(i + LEAD)
        gather(i, w)

    def body(i, _):
        step(i)
        return 0

    step(0, first=True)
    lax.fori_loop(1, shared - LEAD, body, 0)
    for i in range(shared - LEAD, sequences - LEAD):
        step(i)

    send_stats(last)
    send_parts(last - LEAD)
    for i in range(sequences - LEAD, last):
        v_copy(i).wait()
        gather(i, weights[i % (LEAD + 1)])
        send_parts(i)
    w = weights[last % (LEAD + 1)]
    for p in range(PIECES):
        tail_copy(p).wait()
        gather(last, w, few * p, few)
        to_all(last_parts.at[DIRECT - 1, me, p], *tail_of(p))


    def each_round(r, own, other):
        if n * (r + 1) <= shared:
            own(n)
        else:
            pl.when(me < owners)(lambda: own(owners))
            pl.when(me >= owners)(lambda: other(owners))

    for r in range(rounds):

        def sent(count):
            if count:
                wait_for(stats.at[pl.ds(n * r, count)], stat_send.at[r])
                wait_for(parts.at[pl.ds(n * r, count)], part_send.at[r])

        each_round(r, lambda count: sent(count - 1), sent)
    for sem in (last_stat_send, last_stat_recv):
        wait_for(last_stats.at[pl.ds(0, n - 1)], sem)

    for d in range(DIRECT - 1):
        factors = last_scales(d)
        wait_for(last_parts.at[d, pl.ds(0, n - 1)], last_send.at[d])
        wait_for(last_parts.at[d, pl.ds(0, n - 1)], last_recv.at[d])
        join_packed(shared + d, factors)
    d = DIRECT - 1
    factors = last_scales(d)
    for p in range(PIECES):
        for sem in tail_of(p):
            wait_for(last_parts.at[d, pl.ds(0, n - 1), p], sem)
    join_packed(last, factors)

    for r in range(rounds):

        def sent(count):
            wait_for(out.at[pl.ds(0, n - 1)], out_send.at[r])
            wait_for(out.at[pl.ds(0, count - 1)], out_recv.at[r])

        each_round(r, sent, lambda count: wait_for(out.at[pl.ds(0, count)], out_recv.at[r]))


def attend(n, q, k, v):
    sequences, heads, head = q.shape
    tokens, groups = k.shape[1:3]
    width = groups * head
    rounds = -(-(sequences - DIRECT) // n)
    k, v = (jnp.transpose(x, (0, 2, 3, 1)).reshape(sequences, width, tokens) for x in (k, v))
    return pl.pallas_call(
        functools.partial(kernel, n, groups),
        out_shape=pltpu.VMEM(q.shape, q.dtype),
        in_specs=[pl.BlockSpec(memory_space=pl.ANY)] * 3,
        out_specs=pl.BlockSpec(memory_space=pltpu.VMEM),
        scratch_shapes=[
            pltpu.VMEM((sequences * heads, head), jnp.bfloat16),
            pltpu.VMEM((head, width), jnp.bfloat16),
            pltpu.VMEM((heads, width), jnp.bfloat16),
            pltpu.VMEM((sequences * heads, width), jnp.bfloat16),
            pltpu.VMEM((RING, width, tokens), jnp.bfloat16),
            pltpu.VMEM((RING, width, tokens), jnp.bfloat16),
            pltpu.VMEM((LEAD + 1, heads, tokens), jnp.bfloat16),
            pltpu.VMEM((sequences - DIRECT, heads, 2 * LANES), jnp.bfloat16),
            pltpu.VMEM((sequences - DIRECT, 8, LANES), jnp.float32),
            pltpu.VMEM((rounds, n - 1, heads, 2 * LANES), jnp.bfloat16),
            pltpu.VMEM((rounds, n - 1, 8, LANES), jnp.float32),
            pltpu.VMEM((DIRECT, n, PIECES, heads // PIECES + 8, LANES), jnp.bfloat16),
            pltpu.VMEM((n, DIRECT, 1, LANES), jnp.float32),
            pltpu.SemaphoreType.DMA,
            pltpu.SemaphoreType.DMA((RING,)),
            pltpu.SemaphoreType.DMA((RING,)),
            pltpu.SemaphoreType.DMA((PIECES,)),
            *[pltpu.SemaphoreType.DMA((rounds,))] * 6,
            *[pltpu.SemaphoreType.DMA((DIRECT + PIECES - 1,))] * 2,
            *[pltpu.SemaphoreType.DMA] * 2,
        ],
        compiler_params=pltpu.CompilerParams(collective_id=0, has_side_effects=True, vmem_limit_bytes=56 * 2**20),
        name="attend",
    )(q.reshape(sequences * heads, head), k, v)


def solution(mesh):
    return jax.shard_map(
        functools.partial(attend, mesh.shape["sp"]),
        mesh=mesh,
        in_specs=(P("dp", None, None), P("dp", "sp", None, None), P("dp", "sp", None, None)),
        out_specs=P("dp", None, None),
        check_vma=False,
    )
```
